32 devices in a mesh: dp: 16 (over z, x, core), cls: 2 (over y).
Axes of the slice: x: 2, y: 2, z: 4, core: 2. Of those that a mesh axis runs over, the one named last changes fastest.
Arguments:
- features: bfloat16 [512, 65536], P('cls', 'dp'), may hold values from -200 to 200
- labels: int32 [65536], P('dp'), may hold values from 0 to 7
- coeffs: bfloat16 [8, 512], P('cls'), may hold values from -0.176776695 to 0.176776695
- smoothing: float32 [8], replicated, may hold values from 0.1 to 1
- pair_slots: int32 [36], P('cls'), may hold values from 0 to 35, each once
Outputs:
- hessian: float32 [512, 36, 512], P('dp', 'cls')
- gradient: float32 [8, 512], P('cls', 'dp')
The draws below stay inside these ranges and needn't reach their ends.
Inputs may be any that keep to these rules, and one draw needn't show every extreme that they name: `pair_slots`: the entry of slot s of the index c of cls is entry c * 18 + s; an entry below 36 names that pair block, a larger entry marks an empty slot; every value appears once.
All inputs are finite; a program needn't handle non-finite values.
Results may differ from the reference program's by a relative error of at most 0.0003.
Values may be sent and summed in bfloat16 or wider, within the bound.
A program may use at most 256 MiB of HBM per device.

```python
import math
import jax
import jax.numpy as jnp
import numpy as np
from jax import lax

CLASSES = 8
BASIS = 512
ROWS_DEV = 4096
ROWS = 65536
PAIRS = 36
SLOTS = 18
N_CLS = 2


def coeff_table(key):
    values = jax.random.truncated_normal(jax.random.fold_in(key, 11), -4.0, 4.0, (CLASSES, BASIS), jnp.float32)
    return values / math.sqrt(BASIS)


def draw_coeffs(key, part):
    return coeff_table(key).astype(jnp.bfloat16)


def draw_features(key, part):
    values = jax.random.truncated_normal(jax.random.fold_in(key, 12), -6.0, 6.0, (ROWS, BASIS), jnp.float32)
    return jnp.clip(values, -200.0, 200.0).T.astype(jnp.bfloat16)


def place_ends(entries, key, low, top_value):
    spot = [jax.random.randint(jax.random.fold_in(key, axis), (), 0, length) for axis, length in enumerate(entries.shape)]
    widest = entries.shape.index(max(entries.shape))
    beside = spot[:widest] + [(spot[widest] + 1) % entries.shape[widest]] + spot[widest + 1:]
    return entries.at[tuple(spot)].set(low).at[tuple(beside)].set(top_value)


def setup_inputs(seed: int = 0) -> dict:
    seeds = jax.random.split(jax.random.key(seed), 6)
    features = draw_features(jax.random.fold_in(seeds[5], 71), 0)
    labels = place_ends(jax.random.randint(seeds[1], (ROWS,), 0, CLASSES), jax.random.fold_in(seeds[1], 1), 0, CLASSES - 1).astype(jnp.int32)
    coeffs = draw_coeffs(jax.random.fold_in(seeds[5], 71), 0)
    smoothing = jnp.clip(jnp.exp(jax.random.uniform(seeds[3], (CLASSES,), jnp.float32, math.log(0.1), math.log(1.0))), 0.1, 1.0)
    pair_slots = jax.random.permutation(seeds[4], N_CLS * SLOTS).astype(jnp.int32)
    return dict(features=features, labels=labels, coeffs=coeffs, smoothing=smoothing, pair_slots=pair_slots)


def pair_tables():
    first_list = []
    second_list = []
    for class_one in range(CLASSES):
        for class_two in range(class_one, CLASSES):
            first_list.append(class_one)
            second_list.append(class_two)
    return np.array(first_list, np.int32), np.array(second_list, np.int32)


def second_differences(width):
    index_row = jnp.arange(width - 2)[:, None]
    index_col = jnp.arange(width)[None, :]
    return ((index_col == index_row).astype(jnp.float32) - 2.0 * (index_col == index_row + 1).astype(jnp.float32)
            + (index_col == index_row + 2).astype(jnp.float32))


def reference(features, labels, coeffs, smoothing, pair_slots):
    matrix = features.T
    scores = jnp.dot(matrix, coeffs.T, preferred_element_type=jnp.float32)
    row_top = jnp.max(scores, axis=1, keepdims=True)
    exponent = jnp.exp(scores - row_top)
    probs = exponent / jnp.sum(exponent, axis=1, keepdims=True)
    differences = second_differences(BASIS)
    penalty_matrix = jnp.dot(differences.T, differences, precision=lax.Precision.HIGHEST,
                             preferred_element_type=jnp.float32)
    first_tab, second_tab = pair_tables()
    first_tab = jnp.asarray(first_tab)
    second_tab = jnp.asarray(second_tab)
    row_weight = 1.0 / ROWS_DEV

    def pair_block(pair_number):
        class_one = first_tab[pair_number]
        class_two = second_tab[pair_number]
        same_class = (class_one == class_two).astype(jnp.float32)
        prob_one = jnp.take(probs, class_one, axis=1)
        prob_two = jnp.take(probs, class_two, axis=1)
        weights = prob_one * (same_class - prob_two)
        scaled = (matrix * weights[:, None]).astype(jnp.bfloat16)
        products = jnp.dot(scaled.T, matrix, preferred_element_type=jnp.float32) * row_weight
        return products + same_class * smoothing[class_one] * penalty_matrix

    blocks = lax.map(pair_block, jnp.arange(PAIRS, dtype=jnp.int32))
    live_slot = (pair_slots < PAIRS).astype(jnp.float32)
    pair_index = jnp.minimum(pair_slots, PAIRS - 1).astype(jnp.int32)
    chosen = blocks[pair_index] * live_slot[:, None, None]
    hessian = jnp.transpose(chosen, (1, 0, 2))
    one_hot = (labels[:, None] == jnp.arange(CLASSES, dtype=jnp.int32)[None, :]).astype(jnp.float32)
    resid = (one_hot - probs).astype(jnp.bfloat16)
    data_part = jnp.dot(resid.T, matrix, preferred_element_type=jnp.float32) * row_weight
    penalty_part = jnp.dot(coeffs.astype(jnp.float32), penalty_matrix, precision=lax.Precision.HIGHEST,
                           preferred_element_type=jnp.float32)
    gradient = data_part - smoothing[:, None] * penalty_part
    return hessian, gradient
```

```python
import functools
import jax
import jax.numpy as jnp
from jax import lax
from jax.experimental import pallas as pl
from jax.experimental.pallas import tpu as pltpu
from jax.sharding import PartitionSpec as P

CLASSES = 8


def pair_tables():
    first_list = []
    second_list = []
    for class_one in range(CLASSES):
        for class_two in range(class_one, CLASSES):
            first_list.append(class_one)
            second_list.append(class_two)
    return (jnp.array(first_list, jnp.int32), jnp.array(second_list, jnp.int32))


def second_differences(width):
    index_row = jnp.arange(width - 2)[:, None]
    index_col = jnp.arange(width)[None, :]
    return (
        (index_col == index_row).astype(jnp.float32)
        - 2.0 * (index_col == index_row + 1).astype(jnp.float32)
        + (index_col == index_row + 2).astype(jnp.float32)
    )


SLOT_GROUP = 3


def exchange_rows(features):
    parts = lax.axis_size("cls")
    if parts != 2:
        return lax.all_gather(features, "cls", axis=0, tiled=True)
    other = lax.ppermute(features, "cls", [(0, 1), (1, 0)])
    is_low = lax.axis_index("cls") == 0
    low = jnp.where(is_low, features, other)
    high = jnp.where(is_low, other, features)
    return jnp.concatenate([low, high], axis=0)


def halves(array, axis, mine):
    zero = lax.index_in_dim(array, 0, axis, False)
    one = lax.index_in_dim(array, 1, axis, False)
    stays_low = mine == 0
    return jnp.where(stays_low, zero, one), jnp.where(stays_low, one, zero)


class GroupSum:
    def __init__(self, blocks, swap):
        self.owners = lax.axis_size("dp")
        self.bits = self.owners.bit_length() - 1
        self.share = blocks[0].shape[0] // self.owners
        self.order = list(range(self.bits))
        if swap and self.bits > 2:
            self.order[1], self.order[2] = self.order[2], self.order[1]
        self.left = list(range(self.bits - 1, -1, -1))
        self.blocks = blocks
        self.held = None
        self.kept = None
        self.moving = None

    def launch(self):
        if not self.order:
            return
        bit = self.order.pop(0)
        axis = self.left.index(bit)
        self.left.remove(bit)
        mine = (lax.axis_index("dp") >> bit) & 1
        if self.held is None:
            shape = (2,) * self.bits + (self.share, self.blocks[0].shape[1])
            parts = [halves(block.reshape(shape), axis, mine) for block in self.blocks]
            self.kept = jnp.stack([part[0] for part in parts], axis=0)
            sent = jnp.stack([part[1] for part in parts], axis=0)
        else:
            self.kept, sent = halves(self.held, axis + 1, mine)
        pairs = [(owner, owner ^ (1 << bit)) for owner in range(self.owners)]
        self.moving = lax.ppermute(sent, "dp", pairs)

    def land(self):
        if self.moving is None:
            return
        self.held = self.kept + self.moving
        self.moving = None
        self.launch()

    def finish(self):
        if self.owners != 1 << self.bits:
            stacked = jnp.stack(self.blocks, axis=0)
            return lax.psum_scatter(stacked, "dp", scatter_dimension=1, tiled=True)
        while self.moving is not None:
            self.land()
        return self.held


def local(features, labels, coeffs, smoothing, pair_slots):
    row_count = features.shape[1]
    own_width = features.shape[0]
    width = own_width * lax.axis_size("cls")
    row_share = width // lax.axis_size("dp")
    local_classes = coeffs.shape[0]
    slot_count = pair_slots.shape[0]
    row_weight = 1.0 / row_count
    cls_index = lax.axis_index("cls")
    gathered = exchange_rows(features)
    every_coeff = lax.all_gather(coeffs, "cls", axis=0, tiled=True)
    own_coeff = lax.dynamic_slice_in_dim(every_coeff, cls_index * own_width, own_width, 1)
    scores = lax.psum(
        jnp.dot(own_coeff, features, preferred_element_type=jnp.float32), "cls"
    )
    exponent = jnp.exp(scores - jnp.max(scores, axis=0)[None, :])
    every_prob = exponent / jnp.sum(exponent, axis=0)[None, :]
    class_start = cls_index * local_classes
    probs = lax.dynamic_slice_in_dim(every_prob, class_start, local_classes, 0)
    own_classes = class_start + jnp.arange(local_classes, dtype=jnp.int32)
    one_hot = (labels[None, :] == own_classes[:, None]).astype(jnp.float32)
    resid = (one_hot - probs).astype(jnp.bfloat16)
    grad_term = (
        lax.dot_general(
            resid, gathered, (((1,), (1,)), ((), ())), preferred_element_type=jnp.float32
        )
        * row_weight
    )
    grad_share = lax.psum_scatter(grad_term, "dp", scatter_dimension=1, tiled=True)
    row_start = lax.axis_index("dp") * row_share
    differences = second_differences(width)
    own_columns = lax.dynamic_slice_in_dim(differences, row_start, row_share, 1)
    penalty_rows = jnp.dot(
        own_columns.T,
        differences,
        precision=lax.Precision.HIGHEST,
        preferred_element_type=jnp.float32,
    )
    own_smoothing = lax.dynamic_slice_in_dim(smoothing, class_start, local_classes, 0)
    penalty_part = jnp.dot(
        coeffs.astype(jnp.float32),
        penalty_rows.T,
        precision=lax.Precision.HIGHEST,
        preferred_element_type=jnp.float32,
    )
    gradient = grad_share - own_smoothing[:, None] * penalty_part
    first_tab, second_tab = pair_tables()
    pair_count = first_tab.shape[0]
    live_slot = (pair_slots < pair_count).astype(jnp.float32)
    pair_index = jnp.minimum(pair_slots, pair_count - 1)
    pick_pair = pair_index[:, None] == jnp.arange(pair_count, dtype=jnp.int32)[None, :]
    first_class = jnp.sum(jnp.where(pick_pair, first_tab[None, :], 0), axis=1)
    second_class = jnp.sum(jnp.where(pick_pair, second_tab[None, :], 0), axis=1)
    class_range = jnp.arange(CLASSES, dtype=jnp.int32)[None, :]
    select_first = (first_class[:, None] == class_range).astype(jnp.float32)
    select_second = (second_class[:, None] == class_range).astype(jnp.float32)
    prob_first = jnp.dot(
        select_first,
        every_prob,
        precision=lax.Precision.HIGHEST,
        preferred_element_type=jnp.float32,
    )
    prob_second = jnp.dot(
        select_second,
        every_prob,
        precision=lax.Precision.HIGHEST,
        preferred_element_type=jnp.float32,
    )
    same_class = (first_class == second_class).astype(jnp.float32)
    weights = live_slot[:, None] * (prob_first * (same_class[:, None] - prob_second))
    groups = []
    power_of_two = lax.axis_size("dp") & (lax.axis_size("dp") - 1) == 0
    for number, start in enumerate(range(0, slot_count, SLOT_GROUP)):
        if power_of_two:
            for back in (5, 2):
                if number >= back:
                    earlier = groups[number - back]
                    earlier.land()
                    weights, earlier.held, earlier.kept = lax.optimization_barrier(
                        (weights, earlier.held, earlier.kept)
                    )
        blocks = []
        for slot in range(start, min(start + SLOT_GROUP, slot_count)):
            scaled = (gathered * weights[slot][None, :]).astype(jnp.bfloat16)
            blocks.append(
                lax.dot_general(
                    scaled,
                    gathered,
                    (((1,), (1,)), ((), ())),
                    preferred_element_type=jnp.float32,
                )
            )
        groups.append(GroupSum(blocks, number % 2 == 1))
        if power_of_two:
            groups[-1].launch()
    sums = [group.finish() for group in groups]
    own_rows = jnp.transpose(jnp.concatenate(sums, axis=0), (1, 0, 2)) * row_weight
    slot_smoothing = jnp.dot(
        select_first, smoothing, precision=lax.Precision.HIGHEST, preferred_element_type=jnp.float32
    )
    penalty = live_slot * same_class * slot_smoothing
    hessian = (
        own_rows
        + penalty[None, :, None] * penalty_rows[:, None, :]
    )
    return (hessian, gradient)


f32 = jnp.float32
bf16 = jnp.bfloat16
GROUP = 4
LANES = 128
TOP = 32767.0
OFF_PAIRS = [(j, k) for j in range(CLASSES) for k in range(j + 1, CLASSES)]
OFF_INDEX = {pair: e for e, pair in enumerate(OFF_PAIRS)}
N_OFF = len(OFF_PAIRS)
N_GROUPS = N_OFF // GROUP
N_CHUNKS = 2 * N_GROUPS
LAG_X, LAG_Z0, LAG_Z1, LAG_Y, LAG_F, LAG_G = 1, 3, 5, 7, 9, 11


def slot_places():
    places = []
    for j in range(CLASSES):
        for k in range(j, CLASSES):
            places.append(N_OFF + j if j == k else OFF_INDEX[(j, k)])
    return places


def encode(value, axes):
    top = jnp.max(jnp.abs(value), axis=axes, keepdims=True)
    inverse = TOP / jnp.maximum(top, 1e-30)
    code = jnp.round(value * inverse).astype(jnp.int32).astype(jnp.int16)
    return code, top * (1.0 / TOP)


def decode(code, scale):
    return code.astype(jnp.int32).astype(f32) * scale


def kernel_body(
    x_hbm, labels_ref, coeff_ref, smooth_ref, slots_ref, place_ref,
    hess_ref, grad_ref,
    x, xt, xh, xht, cf, part, sc, wts, resid,
    p_buf, rc, k1, sx, sxs, rx, rxs, k2, sz0, sz0s, rz0, rz0s, k3,
    sz1, sz1s, rz1, rz1s, ry, own_b, cross_b, fs, fss, fr, frs, gs, gr,
    load_sem, cf_sem, sc_sem, ft_sem, core_sem, x_sem, xs_sem, z0_sem, z0s_sem,
    z1_sem, z1s_sem, y_sem, f_sem, fsc_sem, g_sem,
):
    width, rows = x.shape
    half = rows // 2
    slab = width // 8
    d = lax.axis_index("dp")
    c = lax.axis_index("cls")
    other = 1 - c
    core = d % 2
    xb = (d // 2) % 2
    z0 = (d // 4) % 2
    z1 = d // 8
    s = d % 8
    peers = {
        "core": d + 1 - 2 * core,
        "x": d + 2 - 4 * xb,
        "z0": d + 4 - 8 * z0,
        "z1": d + 8 - 16 * z1,
    }

    load = pltpu.make_async_copy(x_hbm, x, load_sem)
    load.start()

    mesh_id = pl.DeviceIdType.MESH

    def copy(src, dst, sems, target, *index):
        send, recv = sems.at[0], sems.at[1]
        for i in index:
            send, recv = send.at[i], recv.at[i]
        return pltpu.make_async_remote_copy(
            src_ref=src, dst_ref=dst, send_sem=send, recv_sem=recv,
            device_id=target, device_id_type=mesh_id,
        )

    barrier = pltpu.get_barrier_semaphore()
    for name in ("core", "x", "z0"):
        pl.semaphore_signal(barrier, inc=1, device_id={"dp": peers[name]}, device_id_type=mesh_id)
    for t in range(8):
        pl.semaphore_signal(barrier, inc=1, device_id={"dp": (1 - z1) * 8 + t}, device_id_type=mesh_id)
    pl.semaphore_signal(barrier, inc=1, device_id={"cls": other}, device_id_type=mesh_id)
    n_local = coeff_ref.shape[0]
    cf[c, pl.ds(0, n_local), :] = coeff_ref[...].astype(f32)
    pl.semaphore_wait(barrier, 12)

    to_y = {"cls": other}
    cf_copy = copy(cf.at[c], cf.at[c], cf_sem, to_y)
    cf_copy.start()
    load.wait()
    cf_copy.wait_recv()

    own_cols = pl.ds(pl.multiple_of(c * width, LANES), width)
    coeffs = jnp.concatenate([cf[0, :n_local, :], cf[1, :n_local, :]], axis=0)
    part[...] = coeffs
    own_coeff = part[:, own_cols].astype(bf16)
    sc[c] = jnp.dot(own_coeff, x[...], preferred_element_type=f32)
    sc_copy = copy(sc.at[c], sc.at[c], sc_sem, to_y)
    sc_copy.start()
    sent_obs = pl.ds(pl.multiple_of(other * half, LANES), half)
    ft_copy = copy(x.at[:, sent_obs], xh.at[c], ft_sem, to_y)
    ft_copy.start()

    step = 512

    def flip(i, carry):
        at = pl.ds(pl.multiple_of(i * step, step), step)
        xt[at, :] = x[:, at].T
        return carry

    lax.fori_loop(0, rows // step, flip, 0)
    own_obs = pl.ds(pl.multiple_of(c * half, LANES), half)
    keep_x = pltpu.make_async_copy(x.at[:, own_obs], xh.at[c], load_sem)
    keep_x.start()
    keep_x.wait()
    keep_t = pltpu.make_async_copy(xt.at[own_obs, :], xht.at[c], load_sem)
    keep_t.start()
    keep_t.wait()

    sc_copy.wait_recv()
    scores = sc[0] + sc[1]
    exponent = jnp.exp(scores - jnp.max(scores, axis=0, keepdims=True))
    probs = exponent / jnp.sum(exponent, axis=0, keepdims=True)
    for e, (j, k) in enumerate(OFF_PAIRS):
        wts[e : e + 1, :] = -(probs[j : j + 1, :] * probs[k : k + 1, :])
    classes = lax.broadcasted_iota(jnp.int32, (CLASSES, rows), 0)
    hot = (labels_ref[...] == classes).astype(f32)
    resid[...] = (hot - probs).astype(bf16)

    def is_own(j):
        return j < N_GROUPS

    def group_of(j):
        return jnp.where(j < N_GROUPS, j, j - N_GROUPS)

    def holder(j):
        return jnp.where(j < N_GROUPS, c, (j - N_GROUPS) % 2)

    def core_copy(j):
        return copy(p_buf.at[j, :, :, :, 1 - core], rc.at[j], core_sem, {"dp": peers["core"]}, j)

    def x_copies(j):
        to = {"dp": peers["x"]}
        return copy(sx.at[j], rx.at[j], x_sem, to, j), copy(sxs.at[j], rxs.at[j], xs_sem, to, j)

    def z0_copies(j):
        to = {"dp": peers["z0"]}
        return copy(sz0.at[j], rz0.at[j], z0_sem, to, j), copy(sz0s.at[j], rz0s.at[j], z0s_sem, to, j)

    def z1_copies(j):
        to = {"dp": peers["z1"]}
        return copy(sz1.at[j], rz1.at[j], z1_sem, to, j), copy(sz1s.at[j], rz1s.at[j], z1s_sem, to, j)

    def own_copy(g):
        at = pl.ds(g * GROUP, GROUP)
        return copy(own_b.at[at], own_b.at[at], y_sem, to_y, g)

    def cross_copy(g):
        return copy(k3.at[g + N_GROUPS], ry.at[g], y_sem, to_y, g + N_GROUPS)

    def f_copies(g, t, source):
        to = {"dp": (1 - z1) * 8 + t}

        def one(src, dst, sems):
            return pltpu.make_async_remote_copy(
                src_ref=src, dst_ref=dst, send_sem=sems.at[0, g, t], recv_sem=sems.at[1, g, source],
                device_id=to, device_id_type=mesh_id,
            )

        return (
            one(fs.at[g, pl.ds(t * slab, slab)], fr.at[g, source], f_sem),
            one(fss.at[g], frs.at[g, source], fsc_sem),
        )

    def compute(i):
        @pl.when(is_own(i))
        def _():
            for p in range(GROUP):
                total = None
                for k in range(2):
                    at = pl.ds(k * half, half)
                    scaled = (x[:, at].astype(f32) * wts[pl.ds(i * GROUP + p, 1), at]).astype(bf16)
                    term = jnp.dot(scaled, xt[at, :], preferred_element_type=f32)
                    total = term if total is None else total + term
                p_buf[i, p] = total.reshape(2, 2, 2, slab, width)

        @pl.when(i == N_GROUPS)
        def _():
            ft_copy.wait_recv()

            def flip_other(n, carry):
                at = pl.ds(pl.multiple_of(n * step, step), step)
                xht[other, at, :] = xh[other, :, at].T
                return carry

            lax.fori_loop(0, half // step, flip_other, 0)

        @pl.when(jnp.logical_not(is_own(i)))
        def _():
            g = i - N_GROUPS
            o = g % 2
            for p in range(GROUP):
                scaled = (xh[o].astype(f32) * wts[pl.ds(g * GROUP + p, 1), own_obs]).astype(bf16)
                total = jnp.dot(scaled, xht[1 - o], preferred_element_type=f32)
                p_buf[i, p] = total.reshape(2, 2, 2, slab, width)

        core_copy(i).start()

    def stage_x(j):
        core_copy(j).wait_recv()
        kept = p_buf[j, :, :, xb, core] + rc[j, :, :, xb]
        k1[j] = kept
        sent = p_buf[j, :, :, 1 - xb, core] + rc[j, :, :, 1 - xb]
        code, scale = encode(sent, (1, 2))
        sx[j] = code
        sxs[j] = scale.reshape(GROUP, width)
        for item in x_copies(j):
            item.start()

    def stage_z0(j):
        for item in x_copies(j):
            item.wait_recv()
        scale = rxs[j].reshape(GROUP, 1, width)
        k2[j] = k1[j, :, z0] + decode(rx[j, :, z0], scale)
        sent = k1[j, :, 1 - z0] + decode(rx[j, :, 1 - z0], scale)
        code, top = encode(sent, (1,))
        sz0[j] = code
        sz0s[j] = top.reshape(GROUP, width)
        for item in z0_copies(j):
            item.start()

    def stage_z1(j):
        for item in z0_copies(j):
            item.wait_recv()
        total = k2[j] + decode(rz0[j], rz0s[j].reshape(GROUP, 1, width))

        @pl.when(z1 == holder(j))
        def _():
            k3[j] = total

        @pl.when(z1 != holder(j))
        def _():
            code, top = encode(total, (1,))
            sz1[j] = code
            sz1s[j] = top.reshape(GROUP, width)
            for item in z1_copies(j):
                item.start()

    def stage_y(j):
        @pl.when(z1 == holder(j))
        def _():
            for item in z1_copies(j):
                item.wait_recv()
            total = k3[j] + decode(rz1[j], rz1s[j].reshape(GROUP, 1, width))

            @pl.when(is_own(j))
            def _():
                own_b[pl.ds(j * GROUP, GROUP)] = total
                own_copy(j).start()

            @pl.when(jnp.logical_not(is_own(j)))
            def _():
                k3[j] = total
                cross_copy(j - N_GROUPS).start()

    def stage_f(j):
        @pl.when(jnp.logical_and(is_own(j), z1 != c))
        def _():
            own_copy(j).wait_recv()

        @pl.when(jnp.logical_and(jnp.logical_not(is_own(j)), z1 == holder(j)))
        def _():
            g = j - N_GROUPS
            cross_copy(g).wait_recv()
            total = k3[j] + ry[g]
            cross_b[pl.ds(g * GROUP, GROUP)] = total
            turned = total.reshape(GROUP * slab, width).T
            code, top = encode(turned, (0,))
            fs[g] = code
            fss[g] = top
            for t in range(8):
                for item in f_copies(g, t, s):
                    item.start()

    def stage_g(j):
        @pl.when(jnp.logical_and(jnp.logical_not(is_own(j)), z1 != holder(j)))
        def _():
            g = j - N_GROUPS
            pieces = []
            for source in range(8):
                for item in f_copies(g, source, source):
                    item.wait_recv()
                pieces.append(decode(fr[g, source], frs[g, source]))
            for p in range(GROUP):
                lanes = slice(p * slab, (p + 1) * slab)
                cross_b[g * GROUP + p] = jnp.concatenate([piece[:, lanes] for piece in pieces], axis=1)

    def g_copy(k):
        to = to_y if k == 4 else {"dp": peers[("core", "x", "z0", "z1")[k]]}
        return copy(gs.at[k], gr.at[k], g_sem, to, k)

    def gradient(i):
        for k in range(6):
            @pl.when(i == 1 + 2 * k)
            def _():
                if k == 0:
                    value = jnp.dot(resid[...], xt[...], preferred_element_type=f32)
                else:
                    g_copy(k - 1).wait_recv()
                    if k < 5:
                        value = gs[k - 1] + gr[k - 1]
                if k < 5:
                    gs[k] = value
                    g_copy(k).start()
                else:
                    grad_ref[:, own_cols] = gs[4]
                    grad_ref[:, pl.ds(pl.multiple_of(other * width, LANES), width)] = gr[4]

    def loop(i, carry):
        @pl.when(i < N_CHUNKS)
        def _():
            compute(i)

        gradient(i)
        for lag, stage in (
            (LAG_X, stage_x), (LAG_Z0, stage_z0), (LAG_Z1, stage_z1),
            (LAG_Y, stage_y), (LAG_F, stage_f), (LAG_G, stage_g),
        ):
            @pl.when(jnp.logical_and(i >= lag, i < lag + N_CHUNKS))
            def _():
                stage(i - lag)
        return carry

    lax.fori_loop(0, N_CHUNKS + LAG_G, loop, 0)

    row_weight = 1.0 / rows
    first_row = d * slab
    index_row = lax.broadcasted_iota(jnp.int32, (slab, 2 * width), 0) + first_row
    index_col = lax.broadcasted_iota(jnp.int32, (slab, 2 * width), 1)
    taps = (1.0, -2.0, 1.0)
    penalty = jnp.zeros((slab, 2 * width), f32)
    for u in range(3):
        inside = jnp.logical_and(index_row >= u, index_row - u < 2 * width - 2)
        for v in range(3):
            hit = jnp.logical_and(inside, index_col == index_row - u + v)
            penalty = penalty + jnp.where(hit, taps[u] * taps[v], 0.0)
    lanes_own = pl.ds(pl.multiple_of(z1 * width, LANES), width)
    lanes_cross = pl.ds(pl.multiple_of((1 - z1) * width, LANES), width)
    hess_ref[:, 0, :] = penalty
    pen_own = hess_ref[:, 0, lanes_own]
    pen_cross = hess_ref[:, 0, lanes_cross]
    for j in range(CLASSES):
        for buf, pen in ((own_b, pen_own), (cross_b, pen_cross)):
            total = None
            for k in range(CLASSES):
                if k != j:
                    value = buf[OFF_INDEX[(min(j, k), max(j, k))]]
                    total = value if total is None else total + value
            buf[N_OFF + j] = pen * (smooth_ref[j] * rows) - total
    own_b[N_OFF + CLASSES] = jnp.zeros((slab, width), f32)
    cross_b[N_OFF + CLASSES] = jnp.zeros((slab, width), f32)
    n_pairs = place_ref.shape[0] - 1
    for slot in range(slots_ref.shape[0]):
        place = place_ref[jnp.minimum(slots_ref[slot], n_pairs)]
        hess_ref[:, slot, lanes_own] = own_b[place] * row_weight
        hess_ref[:, slot, lanes_cross] = cross_b[place] * row_weight

    cf_copy.wait_send()
    sc_copy.wait_send()
    ft_copy.wait_send()
    for k in range(5):
        g_copy(k).wait_send()

    def drain(j, carry):
        core_copy(j).wait_send()
        for item in (*x_copies(j), *z0_copies(j)):
            item.wait_send()

        @pl.when(z1 != holder(j))
        def _():
            for item in z1_copies(j):
                item.wait_send()

        @pl.when(z1 == holder(j))
        def _():
            @pl.when(is_own(j))
            def _():
                own_copy(j).wait_send()

            @pl.when(jnp.logical_not(is_own(j)))
            def _():
                g = j - N_GROUPS
                cross_copy(g).wait_send()
                for t in range(8):
                    for item in f_copies(g, t, s):
                        item.wait_send()
        return carry

    lax.fori_loop(0, N_CHUNKS, drain, 0)


def fused(features, labels, coeffs, smoothing, pair_slots):
    width, rows = features.shape
    slab = width // 8
    half = rows // 2
    places = jnp.array(slot_places() + [N_OFF + CLASSES], jnp.int32)
    i16 = jnp.int16
    sem = pltpu.SemaphoreType.DMA
    n = N_CHUNKS
    scratch = [
        pltpu.VMEM((width, rows), bf16),
        pltpu.VMEM((rows, width), bf16),
        pltpu.VMEM((2, width, half), bf16),
        pltpu.VMEM((2, half, width), bf16),
        pltpu.VMEM((2, 8, 2 * width), f32),
        pltpu.VMEM((CLASSES, 2 * width), f32),
        pltpu.VMEM((2, CLASSES, rows), f32),
        pltpu.VMEM((N_OFF, rows), f32),
        pltpu.VMEM((CLASSES, rows), bf16),
        pltpu.VMEM((n, GROUP, 2, 2, 2, slab, width), f32),
        pltpu.VMEM((n, GROUP, 2, 2, slab, width), f32),
        pltpu.VMEM((n, GROUP, 2, slab, width), f32),
        pltpu.VMEM((n, GROUP, 2, slab, width), i16),
        pltpu.VMEM((n, GROUP, width), f32),
        pltpu.VMEM((n, GROUP, 2, slab, width), i16),
        pltpu.VMEM((n, GROUP, width), f32),
        pltpu.VMEM((n, GROUP, slab, width), f32),
        pltpu.VMEM((n, GROUP, slab, width), i16),
        pltpu.VMEM((n, GROUP, width), f32),
        pltpu.VMEM((n, GROUP, slab, width), i16),
        pltpu.VMEM((n, GROUP, width), f32),
        pltpu.VMEM((n, GROUP, slab, width), f32),
        pltpu.VMEM((n, GROUP, slab, width), i16),
        pltpu.VMEM((n, GROUP, width), f32),
        pltpu.VMEM((n, GROUP, slab, width), i16),
        pltpu.VMEM((n, GROUP, width), f32),
        pltpu.VMEM((N_GROUPS, GROUP, slab, width), f32),
        pltpu.VMEM((N_OFF + CLASSES + 1, slab, width), f32),
        pltpu.VMEM((N_OFF + CLASSES + 1, slab, width), f32),
        pltpu.VMEM((N_GROUPS, width, LANES), i16),
        pltpu.VMEM((N_GROUPS, 1, LANES), f32),
        pltpu.VMEM((N_GROUPS, 8, slab, LANES), i16),
        pltpu.VMEM((N_GROUPS, 8, 1, LANES), f32),
        pltpu.VMEM((5, CLASSES, width), f32),
        pltpu.VMEM((5, CLASSES, width), f32),
        sem, sem((2,)), sem((2,)), sem((2,)),
        sem((2, n)), sem((2, n)), sem((2, n)), sem((2, n)), sem((2, n)),
        sem((2, n)), sem((2, n)), sem((2, n)),
        sem((2, N_GROUPS, 8)), sem((2, N_GROUPS, 8)), sem((2, 5)),
    ]
    vmem = pl.BlockSpec(memory_space=pltpu.VMEM)
    smem = pl.BlockSpec(memory_space=pltpu.SMEM)
    hessian, sums = pl.pallas_call(
        kernel_body,
        out_shape=(
            jax.ShapeDtypeStruct((slab, pair_slots.shape[0], 2 * width), f32),
            jax.ShapeDtypeStruct((CLASSES, 2 * width), f32),
        ),
        in_specs=[pl.BlockSpec(memory_space=pl.ANY), vmem, vmem, smem, smem, smem],
        out_specs=(vmem, vmem),
        scratch_shapes=scratch,
        compiler_params=pltpu.CompilerParams(
            collective_id=0, has_side_effects=True, vmem_limit_bytes=64 * 2**20 - 65536
        ),
        name="newton",
    )(features, labels.reshape(1, rows), coeffs, smoothing, pair_slots, places)
    local_classes = coeffs.shape[0]
    class_start = lax.axis_index("cls") * local_classes
    row_start = lax.axis_index("dp") * slab
    own = lax.dynamic_slice(sums, (class_start, row_start), (local_classes, slab))
    values = coeffs.astype(f32)
    bends = values[:, :-2] - 2.0 * values[:, 1:-1] + values[:, 2:]
    penalty = (
        jnp.pad(bends, ((0, 0), (0, 2)))
        - 2.0 * jnp.pad(bends, ((0, 0), (1, 1)))
        + jnp.pad(bends, ((0, 0), (2, 0)))
    )
    own_penalty = lax.dynamic_slice_in_dim(penalty, row_start, slab, 1)
    own_smoothing = lax.dynamic_slice_in_dim(smoothing, class_start, local_classes, 0)
    gradient = own * (1.0 / rows) - own_smoothing[:, None] * own_penalty
    return hessian, gradient


def step(features, labels, coeffs, smoothing, pair_slots):
    width = features.shape[0]
    fits = lax.axis_size("cls") == 2 and lax.axis_size("dp") == 16
    fits = fits and (width // 8) * GROUP == LANES and N_OFF % GROUP == 0
    fits = fits and features.shape[1] % 1024 == 0
    run = fused if fits else local
    return run(features, labels, coeffs, smoothing, pair_slots)


def solution(mesh):
    return jax.shard_map(
        step,
        mesh=mesh,
        in_specs=(P("cls", "dp"), P("dp"), P("cls", None), P(), P("cls")),
        out_specs=(P("dp", "cls", None), P("cls", "dp")),
        check_vma=False,
    )
```

```python
import functools
import jax
import jax.numpy as jnp
from jax import lax
from jax.experimental import pallas as pl
from jax.experimental.pallas import tpu as pltpu
from jax.sharding import PartitionSpec as P

CLASSES = 8


def pair_tables():
    first_list = []
    second_list = []
    for class_one in range(CLASSES):
        for class_two in range(class_one, CLASSES):
            first_list.append(class_one)
            second_list.append(class_two)
    return (jnp.array(first_list, jnp.int32), jnp.array(second_list, jnp.int32))


def second_differences(width):
    index_row = jnp.arange(width - 2)[:, None]
    index_col = jnp.arange(width)[None, :]
    return (
        (index_col == index_row).astype(jnp.float32)
        - 2.0 * (index_col == index_row + 1).astype(jnp.float32)
        + (index_col == index_row + 2).astype(jnp.float32)
    )


SLOT_GROUP = 3


def exchange_rows(features):
    parts = lax.axis_size("cls")
    if parts != 2:
        return lax.all_gather(features, "cls", axis=0, tiled=True)
    other = lax.ppermute(features, "cls", [(0, 1), (1, 0)])
    is_low = lax.axis_index("cls") == 0
    low = jnp.where(is_low, features, other)
    high = jnp.where(is_low, other, features)
    return jnp.concatenate([low, high], axis=0)


def halves(array, axis, mine):
    zero = lax.index_in_dim(array, 0, axis, False)
    one = lax.index_in_dim(array, 1, axis, False)
    stays_low = mine == 0
    return jnp.where(stays_low, zero, one), jnp.where(stays_low, one, zero)


class GroupSum:
    def __init__(self, blocks, swap):
        self.owners = lax.axis_size("dp")
        self.bits = self.owners.bit_length() - 1
        self.share = blocks[0].shape[0] // self.owners
        self.order = list(range(self.bits))
        if swap and self.bits > 2:
            self.order[1], self.order[2] = self.order[2], self.order[1]
        self.left = list(range(self.bits - 1, -1, -1))
        self.blocks = blocks
        self.held = None
        self.kept = None
        self.moving = None

    def launch(self):
        if not self.order:
            return
        bit = self.order.pop(0)
        axis = self.left.index(bit)
        self.left.remove(bit)
        mine = (lax.axis_index("dp") >> bit) & 1
        if self.held is None:
            shape = (2,) * self.bits + (self.share, self.blocks[0].shape[1])
            parts = [halves(block.reshape(shape), axis, mine) for block in self.blocks]
            self.kept = jnp.stack([part[0] for part in parts], axis=0)
            sent = jnp.stack([part[1] for part in parts], axis=0)
        else:
            self.kept, sent = halves(self.held, axis + 1, mine)
        pairs = [(owner, owner ^ (1 << bit)) for owner in range(self.owners)]
        self.moving = lax.ppermute(sent, "dp", pairs)

    def land(self):
        if self.moving is None:
            return
        self.held = self.kept + self.moving
        self.moving = None
        self.launch()

    def finish(self):
        if self.owners != 1 << self.bits:
            stacked = jnp.stack(self.blocks, axis=0)
            return lax.psum_scatter(stacked, "dp", scatter_dimension=1, tiled=True)
        while self.moving is not None:
            self.land()
        return self.held


def local(features, labels, coeffs, smoothing, pair_slots):
    row_count = features.shape[1]
    own_width = features.shape[0]
    width = own_width * lax.axis_size("cls")
    row_share = width // lax.axis_size("dp")
    local_classes = coeffs.shape[0]
    slot_count = pair_slots.shape[0]
    row_weight = 1.0 / row_count
    cls_index = lax.axis_index("cls")
    gathered = exchange_rows(features)
    every_coeff = lax.all_gather(coeffs, "cls", axis=0, tiled=True)
    own_coeff = lax.dynamic_slice_in_dim(every_coeff, cls_index * own_width, own_width, 1)
    scores = lax.psum(
        jnp.dot(own_coeff, features, preferred_element_type=jnp.float32), "cls"
    )
    exponent = jnp.exp(scores - jnp.max(scores, axis=0)[None, :])
    every_prob = exponent / jnp.sum(exponent, axis=0)[None, :]
    class_start = cls_index * local_classes
    probs = lax.dynamic_slice_in_dim(every_prob, class_start, local_classes, 0)
    own_classes = class_start + jnp.arange(local_classes, dtype=jnp.int32)
    one_hot = (labels[None, :] == own_classes[:, None]).astype(jnp.float32)
    resid = (one_hot - probs).astype(jnp.bfloat16)
    grad_term = (
        lax.dot_general(
            resid, gathered, (((1,), (1,)), ((), ())), preferred_element_type=jnp.float32
        )
        * row_weight
    )
    grad_share = lax.psum_scatter(grad_term, "dp", scatter_dimension=1, tiled=True)
    row_start = lax.axis_index("dp") * row_share
    differences = second_differences(width)
    own_columns = lax.dynamic_slice_in_dim(differences, row_start, row_share, 1)
    penalty_rows = jnp.dot(
        own_columns.T,
        differences,
        precision=lax.Precision.HIGHEST,
        preferred_element_type=jnp.float32,
    )
    own_smoothing = lax.dynamic_slice_in_dim(smoothing, class_start, local_classes, 0)
    penalty_part = jnp.dot(
        coeffs.astype(jnp.float32),
        penalty_rows.T,
        precision=lax.Precision.HIGHEST,
        preferred_element_type=jnp.float32,
    )
    gradient = grad_share - own_smoothing[:, None] * penalty_part
    first_tab, second_tab = pair_tables()
    pair_count = first_tab.shape[0]
    live_slot = (pair_slots < pair_count).astype(jnp.float32)
    pair_index = jnp.minimum(pair_slots, pair_count - 1)
    pick_pair = pair_index[:, None] == jnp.arange(pair_count, dtype=jnp.int32)[None, :]
    first_class = jnp.sum(jnp.where(pick_pair, first_tab[None, :], 0), axis=1)
    second_class = jnp.sum(jnp.where(pick_pair, second_tab[None, :], 0), axis=1)
    class_range = jnp.arange(CLASSES, dtype=jnp.int32)[None, :]
    select_first = (first_class[:, None] == class_range).astype(jnp.float32)
    select_second = (second_class[:, None] == class_range).astype(jnp.float32)
    prob_first = jnp.dot(
        select_first,
        every_prob,
        precision=lax.Precision.HIGHEST,
        preferred_element_type=jnp.float32,
    )
    prob_second = jnp.dot(
        select_second,
        every_prob,
        precision=lax.Precision.HIGHEST,
        preferred_element_type=jnp.float32,
    )
    same_class = (first_class == second_class).astype(jnp.float32)
    weights = live_slot[:, None] * (prob_first * (same_class[:, None] - prob_second))
    groups = []
    power_of_two = lax.axis_size("dp") & (lax.axis_size("dp") - 1) == 0
    for number, start in enumerate(range(0, slot_count, SLOT_GROUP)):
        if power_of_two:
            for back in (5, 2):
                if number >= back:
                    earlier = groups[number - back]
                    earlier.land()
                    weights, earlier.held, earlier.kept = lax.optimization_barrier(
                        (weights, earlier.held, earlier.kept)
                    )
        blocks = []
        for slot in range(start, min(start + SLOT_GROUP, slot_count)):
            scaled = (gathered * weights[slot][None, :]).astype(jnp.bfloat16)
            blocks.append(
                lax.dot_general(
                    scaled,
                    gathered,
                    (((1,), (1,)), ((), ())),
                    preferred_element_type=jnp.float32,
                )
            )
        groups.append(GroupSum(blocks, number % 2 == 1))
        if power_of_two:
            groups[-1].launch()
    sums = [group.finish() for group in groups]
    own_rows = jnp.transpose(jnp.concatenate(sums, axis=0), (1, 0, 2)) * row_weight
    slot_smoothing = jnp.dot(
        select_first, smoothing, precision=lax.Precision.HIGHEST, preferred_element_type=jnp.float32
    )
    penalty = live_slot * same_class * slot_smoothing
    hessian = (
        own_rows
        + penalty[None, :, None] * penalty_rows[:, None, :]
    )
    return (hessian, gradient)


f32 = jnp.float32
bf16 = jnp.bfloat16
GROUP = 4
LANES = 128
TOP = 32767.0
OFF_PAIRS = [(j, k) for j in range(CLASSES) for k in range(j + 1, CLASSES)]
OFF_INDEX = {pair: e for e, pair in enumerate(OFF_PAIRS)}
N_OFF = len(OFF_PAIRS)
N_GROUPS = N_OFF // GROUP
N_CHUNKS = 2 * N_GROUPS
OWN_LAST = 1
OWN_FIRST = N_GROUPS - OWN_LAST
LAG_X, LAG_Z0, LAG_Z1, LAG_Y, LAG_F, LAG_G = 1, 3, 4, 6, 8, 16


def slot_places():
    places = []
    for j in range(CLASSES):
        for k in range(j, CLASSES):
            places.append(N_OFF + j if j == k else OFF_INDEX[(j, k)])
    return places


def encode(value, axes):
    top = jnp.max(jnp.abs(value), axis=axes, keepdims=True)
    inverse = TOP / jnp.maximum(top, 1e-30)
    code = jnp.round(value * inverse).astype(jnp.int32).astype(jnp.int16)
    return code, top * (1.0 / TOP)


def decode(code, scale):
    return code.astype(jnp.int32).astype(f32) * scale


def kernel_body(
    x_hbm, labels_ref, coeff_ref, smooth_ref, slots_ref, place_ref,
    hess_ref, grad_ref,
    x, xt, xh, xht, cf, part, sc, wts, resid,
    p_buf, rc, k1, sx, sxs, rx, rxs, k2, sz0, sz0s, rz0, rz0s, k3,
    sz1, sz1s, rz1, rz1s, sy, sys_, ry, rys, own_b, cross_b, fs, fss, fr, frs, gs, gr,
    load_sem, cf_sem, sc_sem, ft_sem, core_sem, x_sem, xs_sem, z0_sem, z0s_sem,
    z1_sem, z1s_sem, y_sem, ys_sem, f_sem, fsc_sem, g_sem,
):
    width, rows = x.shape
    half = rows // 2
    slab = width // 8
    d = lax.axis_index("dp")
    c = lax.axis_index("cls")
    other = 1 - c
    core = d % 2
    xb = (d // 2) % 2
    z0 = (d // 4) % 2
    z1 = d // 8
    s = d % 8
    peers = {
        "core": d + 1 - 2 * core,
        "x": d + 2 - 4 * xb,
        "z0": d + 4 - 8 * z0,
        "z1": d + 8 - 16 * z1,
    }

    load = pltpu.make_async_copy(x_hbm, x, load_sem)
    load.start()

    mesh_id = pl.DeviceIdType.MESH

    def copy(src, dst, sems, target, *index):
        send, recv = sems.at[0], sems.at[1]
        for i in index:
            send, recv = send.at[i], recv.at[i]
        return pltpu.make_async_remote_copy(
            src_ref=src, dst_ref=dst, send_sem=send, recv_sem=recv,
            device_id=target, device_id_type=mesh_id,
        )

    def pooled(src, dst, sems, target, j):
        return pltpu.make_async_remote_copy(
            src_ref=src, dst_ref=dst, send_sem=sems.at[N_CHUNKS], recv_sem=sems.at[j],
            device_id=target, device_id_type=mesh_id,
        )

    barrier = pltpu.get_barrier_semaphore()
    for name in ("core", "x", "z0"):
        pl.semaphore_signal(barrier, inc=1, device_id={"dp": peers[name]}, device_id_type=mesh_id)
    for t in range(8):
        pl.semaphore_signal(barrier, inc=1, device_id={"dp": (1 - z1) * 8 + t}, device_id_type=mesh_id)
    pl.semaphore_signal(barrier, inc=1, device_id={"cls": other}, device_id_type=mesh_id)
    n_local = coeff_ref.shape[0]
    cf[c, pl.ds(0, n_local), :] = coeff_ref[...].astype(f32)
    pl.semaphore_wait(barrier, 12)

    to_y = {"cls": other}
    cf_copy = copy(cf.at[c], cf.at[c], cf_sem, to_y)
    cf_copy.start()
    load.wait()
    cf_copy.wait_recv()

    own_cols = pl.ds(pl.multiple_of(c * width, LANES), width)
    coeffs = jnp.concatenate([cf[0, :n_local, :], cf[1, :n_local, :]], axis=0)
    part[...] = coeffs
    own_coeff = part[:, own_cols].astype(bf16)
    sc[c] = jnp.dot(own_coeff, x[...], preferred_element_type=f32)
    sc_copy = copy(sc.at[c], sc.at[c], sc_sem, to_y)
    sc_copy.start()
    sent_obs = pl.ds(pl.multiple_of(other * half, LANES), half)
    ft_copy = copy(x.at[:, sent_obs], xh.at[c], ft_sem, to_y)
    ft_copy.start()

    step = 512

    def flip(i, carry):
        at = pl.ds(pl.multiple_of(i * step, step), step)
        xt[at, :] = x[:, at].T
        return carry

    lax.fori_loop(0, rows // step, flip, 0)
    own_obs = pl.ds(pl.multiple_of(c * half, LANES), half)
    keep_x = pltpu.make_async_copy(x.at[:, own_obs], xh.at[c], load_sem)
    keep_x.start()
    keep_x.wait()
    keep_t = pltpu.make_async_copy(xt.at[own_obs, :], xht.at[c], load_sem)
    keep_t.start()
    keep_t.wait()

    sc_copy.wait_recv()
    scores = sc[0] + sc[1]
    exponent = jnp.exp(scores - jnp.max(scores, axis=0, keepdims=True))
    probs = exponent / jnp.sum(exponent, axis=0, keepdims=True)
    for e, (j, k) in enumerate(OFF_PAIRS):
        wts[e : e + 1, :] = -(probs[j : j + 1, :] * probs[k : k + 1, :])
    classes = lax.broadcasted_iota(jnp.int32, (CLASSES, rows), 0)
    hot = (labels_ref[...] == classes).astype(f32)
    resid[...] = (hot - probs).astype(bf16)


    def is_own(j):
        return jnp.logical_or(j < OWN_FIRST, j >= OWN_FIRST + N_GROUPS)

    def own_group(j):
        return jnp.where(j < OWN_FIRST, j, j - N_GROUPS)

    def cross_group(j):
        return j - OWN_FIRST

    def holder(j):
        return jnp.where(is_own(j), c, cross_group(j) % 2)

    def core_copy(j):
        return pooled(p_buf.at[j, :, :, :, 1 - core], rc.at[j], core_sem, {"dp": peers["core"]}, j)

    def x_copies(j):
        to = {"dp": peers["x"]}
        return pooled(sx.at[j], rx.at[j], x_sem, to, j), pooled(sxs.at[j], rxs.at[j], xs_sem, to, j)

    def z0_copies(j):
        to = {"dp": peers["z0"]}
        return pooled(sz0.at[j], rz0.at[j], z0_sem, to, j), pooled(sz0s.at[j], rz0s.at[j], z0s_sem, to, j)

    def z1_copies(j):
        to = {"dp": peers["z1"]}
        return copy(sz1.at[j], rz1.at[j], z1_sem, to, j), copy(sz1s.at[j], rz1s.at[j], z1s_sem, to, j)

    def y_copies(j):
        return copy(sy.at[j], ry.at[j], y_sem, to_y, j), copy(sys_.at[j], rys.at[j], ys_sem, to_y, j)

    def f_copies(g, t):
        to = {"dp": (1 - z1) * 8 + t}
        return (
            copy(fs.at[g, pl.ds(t * slab, slab)], fr.at[g, s], f_sem, to, g),
            copy(fss.at[g], frs.at[g, s], fsc_sem, to, g),
        )

    def f_batch(g):
        to = {"dp": peers["z1"]}
        return copy(fr.at[g], fr.at[g], f_sem, to, g), copy(frs.at[g], frs.at[g], fsc_sem, to, g)

    def compute(i):
        @pl.when(is_own(i))
        def _():
            g = own_group(i)
            for p in range(GROUP):
                total = None
                for k in range(2):
                    at = pl.ds(k * half, half)
                    scaled = (x[:, at].astype(f32) * wts[pl.ds(g * GROUP + p, 1), at]).astype(bf16)
                    term = jnp.dot(scaled, xt[at, :], preferred_element_type=f32)
                    total = term if total is None else total + term
                p_buf[i, p] = total.reshape(2, 2, 2, slab, width)

        @pl.when(i == OWN_FIRST)
        def _():
            ft_copy.wait_recv()

            def flip_other(n, carry):
                at = pl.ds(pl.multiple_of(n * step, step), step)
                xht[other, at, :] = xh[other, :, at].T
                return carry

            lax.fori_loop(0, half // step, flip_other, 0)

        @pl.when(jnp.logical_not(is_own(i)))
        def _():
            g = cross_group(i)
            o = g % 2
            for p in range(GROUP):
                scaled = (xh[o].astype(f32) * wts[pl.ds(g * GROUP + p, 1), own_obs]).astype(bf16)
                total = jnp.dot(scaled, xht[1 - o], preferred_element_type=f32)
                p_buf[i, p] = total.reshape(2, 2, 2, slab, width)

        core_copy(i).start()

    def stage_x(j):
        core_copy(j).wait_recv()
        kept = p_buf[j, :, :, xb, core] + rc[j, :, :, xb]
        k1[j] = kept
        sent = p_buf[j, :, :, 1 - xb, core] + rc[j, :, :, 1 - xb]
        code, scale = encode(sent, (1, 2))
        sx[j] = code
        sxs[j] = scale.reshape(GROUP, width)
        for item in x_copies(j):
            item.start()

    def stage_z0(j):
        for item in x_copies(j):
            item.wait_recv()
        scale = rxs[j].reshape(GROUP, 1, width)
        k2[j] = k1[j, :, z0] + decode(rx[j, :, z0], scale)
        sent = k1[j, :, 1 - z0] + decode(rx[j, :, 1 - z0], scale)
        code, top = encode(sent, (1,))
        sz0[j] = code
        sz0s[j] = top.reshape(GROUP, width)
        for item in z0_copies(j):
            item.start()

    def stage_z1(j):
        for item in z0_copies(j):
            item.wait_recv()
        total = k2[j] + decode(rz0[j], rz0s[j].reshape(GROUP, 1, width))

        @pl.when(z1 == holder(j))
        def _():
            k3[j] = total

        @pl.when(z1 != holder(j))
        def _():
            code, top = encode(total, (1,))
            sz1[j] = code
            sz1s[j] = top.reshape(GROUP, width)
            for item in z1_copies(j):
                item.start()

    def stage_y(j):
        @pl.when(z1 == holder(j))
        def _():
            for item in z1_copies(j):
                item.wait_recv()
            total = k3[j] + decode(rz1[j], rz1s[j].reshape(GROUP, 1, width))
            code, top = encode(total, (1,))
            sy[j] = code
            sys_[j] = top.reshape(GROUP, width)
            for item in y_copies(j):
                item.start()

            @pl.when(is_own(j))
            def _():
                own_b[pl.ds(own_group(j) * GROUP, GROUP)] = total

            @pl.when(jnp.logical_not(is_own(j)))
            def _():
                k3[j] = total

    def stage_f(j):
        @pl.when(jnp.logical_and(is_own(j), z1 != c))
        def _():
            for item in y_copies(j):
                item.wait_recv()
            own_b[pl.ds(own_group(j) * GROUP, GROUP)] = decode(ry[j], rys[j].reshape(GROUP, 1, width))

        @pl.when(jnp.logical_and(jnp.logical_not(is_own(j)), z1 == holder(j)))
        def _():
            g = cross_group(j)
            for item in y_copies(j):
                item.wait_recv()
            total = k3[j] + decode(ry[j], rys[j].reshape(GROUP, 1, width))
            cross_b[pl.ds(g * GROUP, GROUP)] = total
            turned = total.reshape(GROUP * slab, width).T
            code, top = encode(turned, (0,))
            fs[g] = code
            fss[g] = top
            for t in range(8):
                for item in f_copies(g, t):
                    item.start()

    def stage_g(j):
        @pl.when(jnp.logical_and(jnp.logical_not(is_own(j)), z1 != holder(j)))
        def _():
            g = cross_group(j)
            pieces = []
            for item in f_batch(g):
                item.wait_recv()
            for source in range(8):
                pieces.append(decode(fr[g, source], frs[g, source]))
            for p in range(GROUP):
                lanes = slice(p * slab, (p + 1) * slab)
                cross_b[g * GROUP + p] = jnp.concatenate([piece[:, lanes] for piece in pieces], axis=1)

    def g_copy(k):
        to = to_y if k == 4 else {"dp": peers[("core", "x", "z0", "z1")[k]]}
        return copy(gs.at[k], gr.at[k], g_sem, to, k)

    def finish_gradient():
        values = cf[c, pl.ds(0, n_local), :]
        wide = 2 * width
        column = lax.broadcasted_iota(jnp.int32, values.shape, 1)
        bends = values - 2.0 * pltpu.roll(values, wide - 1, 1) + pltpu.roll(values, wide - 2, 1)
        bends = jnp.where(column < wide - 2, bends, 0.0)
        penalty = bends - 2.0 * pltpu.roll(bends, 1, 1) + pltpu.roll(bends, 2, 1)
        row = lax.broadcasted_iota(jnp.int32, values.shape, 0)
        scale = jnp.zeros(values.shape, f32)
        for r in range(n_local):
            scale = jnp.where(row == r, smooth_ref[c * n_local + r], scale)
        penalty = pltpu.roll(scale * penalty, lax.rem(wide - d * slab, wide), 1)
        sums = jnp.where(z1 == c, gs[4], gr[4])
        sums = pltpu.roll(sums, lax.rem(width - s * slab, width), 1)
        mine = jnp.where(c == 0, sums[:n_local, :slab], sums[n_local:, :slab])
        grad_ref[...] = mine * (1.0 / rows) - penalty[:, :slab]

    def gradient(i):
        for k in range(6):
            @pl.when(i == 1 + 2 * k)
            def _():
                if k == 0:
                    value = jnp.dot(resid[...], xt[...], preferred_element_type=f32)
                else:
                    g_copy(k - 1).wait_recv()
                    if k < 5:
                        value = gs[k - 1] + gr[k - 1]
                if k < 5:
                    gs[k] = value
                    g_copy(k).start()
                else:
                    finish_gradient()

    def drain(j):
        @pl.when(z1 != holder(j))
        def _():
            for item in z1_copies(j):
                item.wait_send()

        @pl.when(z1 == holder(j))
        def _():
            for item in y_copies(j):
                item.wait_send()

            @pl.when(jnp.logical_not(is_own(j)))
            def _():
                for item in f_batch(cross_group(j)):
                    item.wait_send()

    def loop(i, carry):
        @pl.when(i < N_CHUNKS)
        def _():
            compute(i)

        gradient(i)
        for lag, stage in (
            (LAG_X, stage_x), (LAG_Z0, stage_z0), (LAG_Z1, stage_z1),
            (LAG_Y, stage_y), (LAG_F, stage_f), (LAG_F + 2, drain), (LAG_G, stage_g),
        ):
            @pl.when(jnp.logical_and(i >= lag, i < lag + N_CHUNKS))
            def _():
                stage(i - lag)
        return carry

    lax.fori_loop(0, N_CHUNKS + LAG_G, loop, 0)

    row_weight = 1.0 / rows
    first_row = d * slab
    index_row = lax.broadcasted_iota(jnp.int32, (slab, 2 * width), 0) + first_row
    index_col = lax.broadcasted_iota(jnp.int32, (slab, 2 * width), 1)
    taps = (1.0, -2.0, 1.0)
    penalty = jnp.zeros((slab, 2 * width), f32)
    for u in range(3):
        inside = jnp.logical_and(index_row >= u, index_row - u < 2 * width - 2)
        for v in range(3):
            hit = jnp.logical_and(inside, index_col == index_row - u + v)
            penalty = penalty + jnp.where(hit, taps[u] * taps[v], 0.0)
    lanes_own = pl.ds(pl.multiple_of(z1 * width, LANES), width)
    lanes_cross = pl.ds(pl.multiple_of((1 - z1) * width, LANES), width)
    hess_ref[:, 0, :] = penalty
    pen_own = hess_ref[:, 0, lanes_own]
    pen_cross = hess_ref[:, 0, lanes_cross]
    for j in range(CLASSES):
        for buf, pen in ((own_b, pen_own), (cross_b, pen_cross)):
            total = None
            for k in range(CLASSES):
                if k != j:
                    value = buf[OFF_INDEX[(min(j, k), max(j, k))]]
                    total = value if total is None else total + value
            buf[N_OFF + j] = pen * (smooth_ref[j] * rows) - total
    own_b[N_OFF + CLASSES] = jnp.zeros((slab, width), f32)
    cross_b[N_OFF + CLASSES] = jnp.zeros((slab, width), f32)
    n_pairs = place_ref.shape[0] - 1
    for slot in range(slots_ref.shape[0]):
        place = place_ref[jnp.minimum(slots_ref[slot], n_pairs)]
        hess_ref[:, slot, lanes_own] = own_b[place] * row_weight
        hess_ref[:, slot, lanes_cross] = cross_b[place] * row_weight

    cf_copy.wait_send()
    sc_copy.wait_send()
    ft_copy.wait_send()
    for k in range(5):
        g_copy(k).wait_send()


    pools = (
        (rc, core_sem, "core"), (sx, x_sem, "x"), (sxs, xs_sem, "x"),
        (sz0, z0_sem, "z0"), (sz0s, z0s_sem, "z0"),
    )
    for ref, sems, name in pools:
        pooled(ref, ref, sems, {"dp": peers[name]}, 0).wait_send()


def fused(features, labels, coeffs, smoothing, pair_slots):
    width, rows = features.shape
    slab = width // 8
    half = rows // 2
    places = jnp.array(slot_places() + [N_OFF + CLASSES], jnp.int32)
    i16 = jnp.int16
    sem = pltpu.SemaphoreType.DMA
    n = N_CHUNKS
    scratch = [
        pltpu.VMEM((width, rows), bf16),
        pltpu.VMEM((rows, width), bf16),
        pltpu.VMEM((2, width, half), bf16),
        pltpu.VMEM((2, half, width), bf16),
        pltpu.VMEM((2, 8, 2 * width), f32),
        pltpu.VMEM((CLASSES, 2 * width), f32),
        pltpu.VMEM((2, CLASSES, rows), f32),
        pltpu.VMEM((N_OFF, rows), f32),
        pltpu.VMEM((CLASSES, rows), bf16),
        pltpu.VMEM((n, GROUP, 2, 2, 2, slab, width), f32),
        pltpu.VMEM((n, GROUP, 2, 2, slab, width), f32),
        pltpu.VMEM((n, GROUP, 2, slab, width), f32),
        pltpu.VMEM((n, GROUP, 2, slab, width), i16),
        pltpu.VMEM((n, GROUP, width), f32),
        pltpu.VMEM((n, GROUP, 2, slab, width), i16),
        pltpu.VMEM((n, GROUP, width), f32),
        pltpu.VMEM((n, GROUP, slab, width), f32),
        pltpu.VMEM((n, GROUP, slab, width), i16),
        pltpu.VMEM((n, GROUP, width), f32),
        pltpu.VMEM((n, GROUP, slab, width), i16),
        pltpu.VMEM((n, GROUP, width), f32),
        pltpu.VMEM((n, GROUP, slab, width), f32),
        pltpu.VMEM((n, GROUP, slab, width), i16),
        pltpu.VMEM((n, GROUP, width), f32),
        pltpu.VMEM((n, GROUP, slab, width), i16),
        pltpu.VMEM((n, GROUP, width), f32),
        pltpu.VMEM((n, GROUP, slab, width), i16),
        pltpu.VMEM((n, GROUP, width), f32),
        pltpu.VMEM((n, GROUP, slab, width), i16),
        pltpu.VMEM((n, GROUP, width), f32),
        pltpu.VMEM((N_OFF + CLASSES + 1, slab, width), f32),
        pltpu.VMEM((N_OFF + CLASSES + 1, slab, width), f32),
        pltpu.VMEM((N_GROUPS, width, LANES), i16),
        pltpu.VMEM((N_GROUPS, 1, LANES), f32),
        pltpu.VMEM((N_GROUPS, 8, slab, LANES), i16),
        pltpu.VMEM((N_GROUPS, 8, 1, LANES), f32),
        pltpu.VMEM((5, CLASSES, width), f32),
        pltpu.VMEM((5, CLASSES, width), f32),
        sem, sem((2,)), sem((2,)), sem((2,)),
        sem((n + 1,)), sem((n + 1,)), sem((n + 1,)), sem((n + 1,)), sem((n + 1,)),
        sem((2, n)), sem((2, n)), sem((2, n)), sem((2, n)),
        sem((2, N_GROUPS)), sem((2, N_GROUPS)), sem((2, 5)),
    ]
    vmem = pl.BlockSpec(memory_space=pltpu.VMEM)
    smem = pl.BlockSpec(memory_space=pltpu.SMEM)
    return pl.pallas_call(
        kernel_body,
        out_shape=(
            jax.ShapeDtypeStruct((slab, pair_slots.shape[0], 2 * width), f32),
            jax.ShapeDtypeStruct((coeffs.shape[0], slab), f32),
        ),
        in_specs=[pl.BlockSpec(memory_space=pl.ANY), vmem, vmem, smem, smem, smem],
        out_specs=(vmem, vmem),
        scratch_shapes=scratch,
        compiler_params=pltpu.CompilerParams(
            collective_id=0, has_side_effects=True, vmem_limit_bytes=64 * 2**20 - 65536
        ),
        name="newton",
    )(features, labels.reshape(1, rows), coeffs, smoothing, pair_slots, places)


def step(features, labels, coeffs, smoothing, pair_slots):
    width = features.shape[0]
    fits = lax.axis_size("cls") == 2 and lax.axis_size("dp") == 16
    fits = fits and (width // 8) * GROUP == LANES and N_OFF % GROUP == 0
    fits = fits and features.shape[1] % 1024 == 0
    run = fused if fits else local
    return run(features, labels, coeffs, smoothing, pair_slots)


def solution(mesh):
    return jax.shard_map(
        step,
        mesh=mesh,
        in_specs=(P("cls", "dp"), P("dp"), P("cls", None), P(), P("cls")),
        out_specs=(P("dp", "cls", None), P("cls", "dp")),
        check_vma=False,
    )
```

```python
import functools
import jax
import jax.numpy as jnp
from jax import lax
from jax.experimental import pallas as pl
from jax.experimental.pallas import tpu as pltpu
from jax.sharding import PartitionSpec as P

CLASSES = 8


def pair_tables():
    first_list = []
    second_list = []
    for class_one in range(CLASSES):
        for class_two in range(class_one, CLASSES):
            first_list.append(class_one)
            second_list.append(class_two)
    return (jnp.array(first_list, jnp.int32), jnp.array(second_list, jnp.int32))


def second_differences(width):
    index_row = jnp.arange(width - 2)[:, None]
    index_col = jnp.arange(width)[None, :]
    return (
        (index_col == index_row).astype(jnp.float32)
        - 2.0 * (index_col == index_row + 1).astype(jnp.float32)
        + (index_col == index_row + 2).astype(jnp.float32)
    )


SLOT_GROUP = 3


def exchange_rows(features):
    parts = lax.axis_size("cls")
    if parts != 2:
        return lax.all_gather(features, "cls", axis=0, tiled=True)
    other = lax.ppermute(features, "cls", [(0, 1), (1, 0)])
    is_low = lax.axis_index("cls") == 0
    low = jnp.where(is_low, features, other)
    high = jnp.where(is_low, other, features)
    return jnp.concatenate([low, high], axis=0)


def halves(array, axis, mine):
    zero = lax.index_in_dim(array, 0, axis, False)
    one = lax.index_in_dim(array, 1, axis, False)
    stays_low = mine == 0
    return jnp.where(stays_low, zero, one), jnp.where(stays_low, one, zero)


class GroupSum:
    def __init__(self, blocks, swap):
        self.owners = lax.axis_size("dp")
        self.bits = self.owners.bit_length() - 1
        self.share = blocks[0].shape[0] // self.owners
        self.order = list(range(self.bits))
        if swap and self.bits > 2:
            self.order[1], self.order[2] = self.order[2], self.order[1]
        self.left = list(range(self.bits - 1, -1, -1))
        self.blocks = blocks
        self.held = None
        self.kept = None
        self.moving = None

    def launch(self):
        if not self.order:
            return
        bit = self.order.pop(0)
        axis = self.left.index(bit)
        self.left.remove(bit)
        mine = (lax.axis_index("dp") >> bit) & 1
        if self.held is None:
            shape = (2,) * self.bits + (self.share, self.blocks[0].shape[1])
            parts = [halves(block.reshape(shape), axis, mine) for block in self.blocks]
            self.kept = jnp.stack([part[0] for part in parts], axis=0)
            sent = jnp.stack([part[1] for part in parts], axis=0)
        else:
            self.kept, sent = halves(self.held, axis + 1, mine)
        pairs = [(owner, owner ^ (1 << bit)) for owner in range(self.owners)]
        self.moving = lax.ppermute(sent, "dp", pairs)

    def land(self):
        if self.moving is None:
            return
        self.held = self.kept + self.moving
        self.moving = None
        self.launch()

    def finish(self):
        if self.owners != 1 << self.bits:
            stacked = jnp.stack(self.blocks, axis=0)
            return lax.psum_scatter(stacked, "dp", scatter_dimension=1, tiled=True)
        while self.moving is not None:
            self.land()
        return self.held


def local(features, labels, coeffs, smoothing, pair_slots):
    row_count = features.shape[1]
    own_width = features.shape[0]
    width = own_width * lax.axis_size("cls")
    row_share = width // lax.axis_size("dp")
    local_classes = coeffs.shape[0]
    slot_count = pair_slots.shape[0]
    row_weight = 1.0 / row_count
    cls_index = lax.axis_index("cls")
    gathered = exchange_rows(features)
    every_coeff = lax.all_gather(coeffs, "cls", axis=0, tiled=True)
    own_coeff = lax.dynamic_slice_in_dim(every_coeff, cls_index * own_width, own_width, 1)
    scores = lax.psum(
        jnp.dot(own_coeff, features, preferred_element_type=jnp.float32), "cls"
    )
    exponent = jnp.exp(scores - jnp.max(scores, axis=0)[None, :])
    every_prob = exponent / jnp.sum(exponent, axis=0)[None, :]
    class_start = cls_index * local_classes
    probs = lax.dynamic_slice_in_dim(every_prob, class_start, local_classes, 0)
    own_classes = class_start + jnp.arange(local_classes, dtype=jnp.int32)
    one_hot = (labels[None, :] == own_classes[:, None]).astype(jnp.float32)
    resid = (one_hot - probs).astype(jnp.bfloat16)
    grad_term = (
        lax.dot_general(
            resid, gathered, (((1,), (1,)), ((), ())), preferred_element_type=jnp.float32
        )
        * row_weight
    )
    grad_share = lax.psum_scatter(grad_term, "dp", scatter_dimension=1, tiled=True)
    row_start = lax.axis_index("dp") * row_share
    differences = second_differences(width)
    own_columns = lax.dynamic_slice_in_dim(differences, row_start, row_share, 1)
    penalty_rows = jnp.dot(
        own_columns.T,
        differences,
        precision=lax.Precision.HIGHEST,
        preferred_element_type=jnp.float32,
    )
    own_smoothing = lax.dynamic_slice_in_dim(smoothing, class_start, local_classes, 0)
    penalty_part = jnp.dot(
        coeffs.astype(jnp.float32),
        penalty_rows.T,
        precision=lax.Precision.HIGHEST,
        preferred_element_type=jnp.float32,
    )
    gradient = grad_share - own_smoothing[:, None] * penalty_part
    first_tab, second_tab = pair_tables()
    pair_count = first_tab.shape[0]
    live_slot = (pair_slots < pair_count).astype(jnp.float32)
    pair_index = jnp.minimum(pair_slots, pair_count - 1)
    pick_pair = pair_index[:, None] == jnp.arange(pair_count, dtype=jnp.int32)[None, :]
    first_class = jnp.sum(jnp.where(pick_pair, first_tab[None, :], 0), axis=1)
    second_class = jnp.sum(jnp.where(pick_pair, second_tab[None, :], 0), axis=1)
    class_range = jnp.arange(CLASSES, dtype=jnp.int32)[None, :]
    select_first = (first_class[:, None] == class_range).astype(jnp.float32)
    select_second = (second_class[:, None] == class_range).astype(jnp.float32)
    prob_first = jnp.dot(
        select_first,
        every_prob,
        precision=lax.Precision.HIGHEST,
        preferred_element_type=jnp.float32,
    )
    prob_second = jnp.dot(
        select_second,
        every_prob,
        precision=lax.Precision.HIGHEST,
        preferred_element_type=jnp.float32,
    )
    same_class = (first_class == second_class).astype(jnp.float32)
    weights = live_slot[:, None] * (prob_first * (same_class[:, None] - prob_second))
    groups = []
    power_of_two = lax.axis_size("dp") & (lax.axis_size("dp") - 1) == 0
    for number, start in enumerate(range(0, slot_count, SLOT_GROUP)):
        if power_of_two:
            for back in (5, 2):
                if number >= back:
                    earlier = groups[number - back]
                    earlier.land()
                    weights, earlier.held, earlier.kept = lax.optimization_barrier(
                        (weights, earlier.held, earlier.kept)
                    )
        blocks = []
        for slot in range(start, min(start + SLOT_GROUP, slot_count)):
            scaled = (gathered * weights[slot][None, :]).astype(jnp.bfloat16)
            blocks.append(
                lax.dot_general(
                    scaled,
                    gathered,
                    (((1,), (1,)), ((), ())),
                    preferred_element_type=jnp.float32,
                )
            )
        groups.append(GroupSum(blocks, number % 2 == 1))
        if power_of_two:
            groups[-1].launch()
    sums = [group.finish() for group in groups]
    own_rows = jnp.transpose(jnp.concatenate(sums, axis=0), (1, 0, 2)) * row_weight
    slot_smoothing = jnp.dot(
        select_first, smoothing, precision=lax.Precision.HIGHEST, preferred_element_type=jnp.float32
    )
    penalty = live_slot * same_class * slot_smoothing
    hessian = (
        own_rows
        + penalty[None, :, None] * penalty_rows[:, None, :]
    )
    return (hessian, gradient)


f32 = jnp.float32
bf16 = jnp.bfloat16
GROUP = 2
PACK = 4
JOIN = PACK // GROUP
LANES = 128
TOP = 32767.0
OFF_PAIRS = [(j, k) for j in range(CLASSES) for k in range(j + 1, CLASSES)]
OFF_INDEX = {pair: e for e, pair in enumerate(OFF_PAIRS)}
N_OFF = len(OFF_PAIRS)
N_GROUPS = N_OFF // GROUP
N_CHUNKS = 2 * N_GROUPS
N_PACKS = N_OFF // PACK
OWN_LAST = 0
OWN_FIRST = N_GROUPS - OWN_LAST
LAG_DRAIN = 3
LAG_X, LAG_Z0, LAG_Z1, LAG_Y, LAG_F, LAG_G = 1, 5, 8, 12, 15, 30


def slot_places():
    places = []
    for j in range(CLASSES):
        for k in range(j, CLASSES):
            places.append(N_OFF + j if j == k else OFF_INDEX[(j, k)])
    return places


def encode(value, axes):
    top = jnp.max(jnp.abs(value), axis=axes, keepdims=True)
    inverse = TOP / jnp.maximum(top, 1e-30)
    code = jnp.round(value * inverse).astype(jnp.int32).astype(jnp.int16)
    return code, top * (1.0 / TOP)


def decode(code, scale):
    return code.astype(jnp.int32).astype(f32) * scale


def kernel_body(
    x_hbm, labels_ref, coeff_ref, smooth_ref, slots_ref, place_ref,
    hess_ref, grad_ref,
    x, xt, xh, xht, cf, part, sc, wts, resid,
    p_buf, rc, k1, sx, sxs, rx, rxs, k2, sz0, sz0s, rz0, rz0s, k3,
    sz1, sz1s, rz1, rz1s, sy, sys_, ry, rys, own_b, cross_b, fs, fss, fr, frs, gs, gr,
    load_sem, cf_sem, sc_sem, ft_sem, core_sem, x_sem, xs_sem, z0_sem, z0s_sem,
    z1_sem, z1s_sem, y_sem, ys_sem, f_sem, fsc_sem, g_sem,
):
    width, rows = x.shape
    half = rows // 2
    slab = width // 8
    d = lax.axis_index("dp")
    c = lax.axis_index("cls")
    other = 1 - c
    core = d % 2
    xb = (d // 2) % 2
    z0 = (d // 4) % 2
    z1 = d // 8
    s = d % 8
    peers = {
        "core": d + 1 - 2 * core,
        "x": d + 2 - 4 * xb,
        "z0": d + 4 - 8 * z0,
        "z1": d + 8 - 16 * z1,
    }

    load = pltpu.make_async_copy(x_hbm, x, load_sem)
    load.start()

    mesh_id = pl.DeviceIdType.MESH

    def copy(src, dst, sems, target, *index):
        send, recv = sems.at[0], sems.at[1]
        for i in index:
            send, recv = send.at[i], recv.at[i]
        return pltpu.make_async_remote_copy(
            src_ref=src, dst_ref=dst, send_sem=send, recv_sem=recv,
            device_id=target, device_id_type=mesh_id,
        )

    def pooled(src, dst, sems, target, j):
        return pltpu.make_async_remote_copy(
            src_ref=src, dst_ref=dst, send_sem=sems.at[N_CHUNKS], recv_sem=sems.at[j],
            device_id=target, device_id_type=mesh_id,
        )

    barrier = pltpu.get_barrier_semaphore()
    for name in ("core", "x", "z0"):
        pl.semaphore_signal(barrier, inc=1, device_id={"dp": peers[name]}, device_id_type=mesh_id)
    for t in range(8):
        pl.semaphore_signal(barrier, inc=1, device_id={"dp": (1 - z1) * 8 + t}, device_id_type=mesh_id)
    pl.semaphore_signal(barrier, inc=1, device_id={"cls": other}, device_id_type=mesh_id)
    n_local = coeff_ref.shape[0]
    cf[c, pl.ds(0, n_local), :] = coeff_ref[...].astype(f32)
    pl.semaphore_wait(barrier, 12)

    to_y = {"cls": other}
    cf_copy = copy(cf.at[c], cf.at[c], cf_sem, to_y)
    cf_copy.start()
    load.wait()
    cf_copy.wait_recv()

    own_cols = pl.ds(pl.multiple_of(c * width, LANES), width)
    coeffs = jnp.concatenate([cf[0, :n_local, :], cf[1, :n_local, :]], axis=0)
    part[...] = coeffs
    own_coeff = part[:, own_cols].astype(bf16)
    sc[c] = jnp.dot(own_coeff, x[...], preferred_element_type=f32)
    sc_copy = copy(sc.at[c], sc.at[c], sc_sem, to_y)
    sc_copy.start()
    sent_obs = pl.ds(pl.multiple_of(other * half, LANES), half)
    ft_copy = copy(x.at[:, sent_obs], xh.at[c], ft_sem, to_y)
    ft_copy.start()

    step = 512

    def flip(i, carry):
        at = pl.ds(pl.multiple_of(i * step, step), step)
        xt[at, :] = x[:, at].T
        return carry

    lax.fori_loop(0, rows // step, flip, 0)
    own_obs = pl.ds(pl.multiple_of(c * half, LANES), half)
    keep_x = pltpu.make_async_copy(x.at[:, own_obs], xh.at[c], load_sem)
    keep_x.start()
    keep_x.wait()
    keep_t = pltpu.make_async_copy(xt.at[own_obs, :], xht.at[c], load_sem)
    keep_t.start()
    keep_t.wait()

    sc_copy.wait_recv()
    scores = sc[0] + sc[1]
    exponent = jnp.exp(scores - jnp.max(scores, axis=0, keepdims=True))
    probs = exponent / jnp.sum(exponent, axis=0, keepdims=True)
    for e, (j, k) in enumerate(OFF_PAIRS):
        wts[e : e + 1, :] = -(probs[j : j + 1, :] * probs[k : k + 1, :])
    classes = lax.broadcasted_iota(jnp.int32, (CLASSES, rows), 0)
    hot = (labels_ref[...] == classes).astype(f32)
    resid[...] = (hot - probs).astype(bf16)


    def is_own(j):
        return jnp.logical_or(j < OWN_FIRST, j >= OWN_FIRST + N_GROUPS)

    def own_group(j):
        return jnp.where(j < OWN_FIRST, j, j - N_GROUPS)

    def cross_group(j):
        return j - OWN_FIRST

    def holder(j):
        return jnp.where(is_own(j), c, (cross_group(j) // JOIN) % 2)

    def core_copy(j):
        return pooled(p_buf.at[j, :, :, :, 1 - core], rc.at[j], core_sem, {"dp": peers["core"]}, j)

    def x_copies(j):
        to = {"dp": peers["x"]}
        return pooled(sx.at[j], rx.at[j], x_sem, to, j), pooled(sxs.at[j], rxs.at[j], xs_sem, to, j)

    def z0_copies(j):
        to = {"dp": peers["z0"]}
        return pooled(sz0.at[j], rz0.at[j], z0_sem, to, j), pooled(sz0s.at[j], rz0s.at[j], z0s_sem, to, j)

    def z1_copies(j):
        to = {"dp": peers["z1"]}
        return copy(sz1.at[j], rz1.at[j], z1_sem, to, j), copy(sz1s.at[j], rz1s.at[j], z1s_sem, to, j)

    def y_copies(j):
        return copy(sy.at[j], ry.at[j], y_sem, to_y, j), copy(sys_.at[j], rys.at[j], ys_sem, to_y, j)

    def f_copies(g, t):
        to = {"dp": (1 - z1) * 8 + t}
        return (
            copy(fs.at[g, pl.ds(t * slab, slab)], fr.at[g, s], f_sem, to, g),
            copy(fss.at[g], frs.at[g, s], fsc_sem, to, g),
        )

    def f_batch(g):
        to = {"dp": peers["z1"]}
        return copy(fr.at[g], fr.at[g], f_sem, to, g), copy(frs.at[g], frs.at[g], fsc_sem, to, g)

    def compute(i):
        @pl.when(is_own(i))
        def _():
            g = own_group(i)
            for p in range(GROUP):
                total = None
                for k in range(2):
                    at = pl.ds(k * half, half)
                    scaled = (x[:, at].astype(f32) * wts[pl.ds(g * GROUP + p, 1), at]).astype(bf16)
                    term = jnp.dot(scaled, xt[at, :], preferred_element_type=f32)
                    total = term if total is None else total + term
                p_buf[i, p] = total.reshape(2, 2, 2, slab, width)

        @pl.when(i == OWN_FIRST)
        def _():
            ft_copy.wait_recv()

            def flip_other(n, carry):
                at = pl.ds(pl.multiple_of(n * step, step), step)
                xht[other, at, :] = xh[other, :, at].T
                return carry

            lax.fori_loop(0, half // step, flip_other, 0)

        @pl.when(jnp.logical_not(is_own(i)))
        def _():
            g = cross_group(i)
            o = (g // JOIN) % 2
            for p in range(GROUP):
                scaled = (xh[o].astype(f32) * wts[pl.ds(g * GROUP + p, 1), own_obs]).astype(bf16)
                total = jnp.dot(scaled, xht[1 - o], preferred_element_type=f32)
                p_buf[i, p] = total.reshape(2, 2, 2, slab, width)

        core_copy(i).start()

    def stage_x(j):
        core_copy(j).wait_recv()
        kept = p_buf[j, :, :, xb, core] + rc[j, :, :, xb]
        k1[j] = kept
        sent = p_buf[j, :, :, 1 - xb, core] + rc[j, :, :, 1 - xb]
        code, scale = encode(sent, (1, 2))
        sx[j] = code
        sxs[j] = scale.reshape(GROUP, width)
        for item in x_copies(j):
            item.start()

    def stage_z0(j):
        for item in x_copies(j):
            item.wait_recv()
        scale = rxs[j].reshape(GROUP, 1, width)
        k2[j] = k1[j, :, z0] + decode(rx[j, :, z0], scale)
        sent = k1[j, :, 1 - z0] + decode(rx[j, :, 1 - z0], scale)
        code, top = encode(sent, (1,))
        sz0[j] = code
        sz0s[j] = top.reshape(GROUP, width)
        for item in z0_copies(j):
            item.start()

    def stage_z1(j):
        for item in z0_copies(j):
            item.wait_recv()
        total = k2[j] + decode(rz0[j], rz0s[j].reshape(GROUP, 1, width))

        @pl.when(z1 == holder(j))
        def _():
            k3[j] = total

        @pl.when(z1 != holder(j))
        def _():
            code, top = encode(total, (1,))
            sz1[j] = code
            sz1s[j] = top.reshape(GROUP, width)
            for item in z1_copies(j):
                item.start()

    def stage_y(j):
        @pl.when(z1 == holder(j))
        def _():
            for item in z1_copies(j):
                item.wait_recv()
            total = k3[j] + decode(rz1[j], rz1s[j].reshape(GROUP, 1, width))
            code, top = encode(total, (1,))
            sy[j] = code
            sys_[j] = top.reshape(GROUP, width)
            for item in y_copies(j):
                item.start()

            @pl.when(is_own(j))
            def _():
                own_b[pl.ds(own_group(j) * GROUP, GROUP)] = total

            @pl.when(jnp.logical_not(is_own(j)))
            def _():
                k3[j] = total

    def stage_f(j):
        @pl.when(jnp.logical_and(is_own(j), z1 != c))
        def _():
            for item in y_copies(j):
                item.wait_recv()
            own_b[pl.ds(own_group(j) * GROUP, GROUP)] = decode(ry[j], rys[j].reshape(GROUP, 1, width))

        @pl.when(jnp.logical_and(jnp.logical_not(is_own(j)), z1 == holder(j)))
        def _():
            g = cross_group(j)
            for item in y_copies(j):
                item.wait_recv()
            total = k3[j] + decode(ry[j], rys[j].reshape(GROUP, 1, width))
            cross_b[pl.ds(g * GROUP, GROUP)] = total

            @pl.when(g % JOIN == JOIN - 1)
            def _():
                k = g // JOIN
                turned = cross_b[pl.ds(k * PACK, PACK)].reshape(PACK * slab, width).T
                code, top = encode(turned, (0,))
                fs[k] = code
                fss[k] = top
                for t in range(8):
                    for item in f_copies(k, t):
                        item.start()

    def last_of_pack(j):
        return jnp.logical_and(jnp.logical_not(is_own(j)), cross_group(j) % JOIN == JOIN - 1)

    def stage_g(j):
        @pl.when(jnp.logical_and(last_of_pack(j), z1 != holder(j)))
        def _():
            k = cross_group(j) // JOIN
            pieces = []
            for item in f_batch(k):
                item.wait_recv()
            for source in range(8):
                pieces.append(decode(fr[k, source], frs[k, source]))
            for p in range(PACK):
                lanes = slice(p * slab, (p + 1) * slab)
                cross_b[k * PACK + p] = jnp.concatenate([piece[:, lanes] for piece in pieces], axis=1)

    def g_copy(k):
        to = to_y if k == 4 else {"dp": peers[("core", "x", "z0", "z1")[k]]}
        return copy(gs.at[k], gr.at[k], g_sem, to, k)

    def finish_gradient():
        values = cf[c, pl.ds(0, n_local), :]
        wide = 2 * width
        column = lax.broadcasted_iota(jnp.int32, values.shape, 1)
        bends = values - 2.0 * pltpu.roll(values, wide - 1, 1) + pltpu.roll(values, wide - 2, 1)
        bends = jnp.where(column < wide - 2, bends, 0.0)
        penalty = bends - 2.0 * pltpu.roll(bends, 1, 1) + pltpu.roll(bends, 2, 1)
        row = lax.broadcasted_iota(jnp.int32, values.shape, 0)
        scale = jnp.zeros(values.shape, f32)
        for r in range(n_local):
            scale = jnp.where(row == r, smooth_ref[c * n_local + r], scale)
        penalty = pltpu.roll(scale * penalty, lax.rem(wide - d * slab, wide), 1)
        sums = jnp.where(z1 == c, gs[4], gr[4])
        sums = pltpu.roll(sums, lax.rem(width - s * slab, width), 1)
        mine = jnp.where(c == 0, sums[:n_local, :slab], sums[n_local:, :slab])
        grad_ref[...] = mine * (1.0 / rows) - penalty[:, :slab]

    def gradient(i):
        for k in range(6):
            @pl.when(i == 4 + 3 * k)
            def _():
                if k == 0:
                    value = jnp.dot(resid[...], xt[...], preferred_element_type=f32)
                else:
                    g_copy(k - 1).wait_recv()
                    if k < 5:
                        value = gs[k - 1] + gr[k - 1]
                if k < 5:
                    gs[k] = value
                    g_copy(k).start()
                else:
                    finish_gradient()

    def drain(j):
        @pl.when(z1 != holder(j))
        def _():
            for item in z1_copies(j):
                item.wait_send()

        @pl.when(z1 == holder(j))
        def _():
            for item in y_copies(j):
                item.wait_send()

            @pl.when(last_of_pack(j))
            def _():
                for item in f_batch(cross_group(j) // JOIN):
                    item.wait_send()

    def loop(i, carry):
        @pl.when(i < N_CHUNKS)
        def _():
            compute(i)

        gradient(i)
        for lag, stage in (
            (LAG_X, stage_x), (LAG_Z0, stage_z0), (LAG_Z1, stage_z1),
            (LAG_Y, stage_y), (LAG_F, stage_f), (LAG_F + LAG_DRAIN, drain), (LAG_G, stage_g),
        ):
            @pl.when(jnp.logical_and(i >= lag, i < lag + N_CHUNKS))
            def _():
                stage(i - lag)
        return carry

    lax.fori_loop(0, N_CHUNKS + LAG_G, loop, 0)

    row_weight = 1.0 / rows
    first_row = d * slab
    index_row = lax.broadcasted_iota(jnp.int32, (slab, 2 * width), 0) + first_row
    index_col = lax.broadcasted_iota(jnp.int32, (slab, 2 * width), 1)
    taps = (1.0, -2.0, 1.0)
    penalty = jnp.zeros((slab, 2 * width), f32)
    for u in range(3):
        inside = jnp.logical_and(index_row >= u, index_row - u < 2 * width - 2)
        for v in range(3):
            hit = jnp.logical_and(inside, index_col == index_row - u + v)
            penalty = penalty + jnp.where(hit, taps[u] * taps[v], 0.0)
    lanes_own = pl.ds(pl.multiple_of(z1 * width, LANES), width)
    lanes_cross = pl.ds(pl.multiple_of((1 - z1) * width, LANES), width)
    hess_ref[:, 0, :] = penalty
    pen_own = hess_ref[:, 0, lanes_own]
    pen_cross = hess_ref[:, 0, lanes_cross]
    for j in range(CLASSES):
        for buf, pen in ((own_b, pen_own), (cross_b, pen_cross)):
            total = None
            for k in range(CLASSES):
                if k != j:
                    value = buf[OFF_INDEX[(min(j, k), max(j, k))]]
                    total = value if total is None else total + value
            buf[N_OFF + j] = pen * (smooth_ref[j] * rows) - total
    own_b[N_OFF + CLASSES] = jnp.zeros((slab, width), f32)
    cross_b[N_OFF + CLASSES] = jnp.zeros((slab, width), f32)
    n_pairs = place_ref.shape[0] - 1
    for slot in range(slots_ref.shape[0]):
        place = place_ref[jnp.minimum(slots_ref[slot], n_pairs)]
        hess_ref[:, slot, lanes_own] = own_b[place] * row_weight
        hess_ref[:, slot, lanes_cross] = cross_b[place] * row_weight

    cf_copy.wait_send()
    sc_copy.wait_send()
    ft_copy.wait_send()
    for k in range(5):
        g_copy(k).wait_send()
    pools = (
        (rc, core_sem, "core"), (sx, x_sem, "x"), (sxs, xs_sem, "x"),
        (sz0, z0_sem, "z0"), (sz0s, z0s_sem, "z0"),
    )
    for ref, sems, name in pools:
        pooled(ref, ref, sems, {"dp": peers[name]}, 0).wait_send()


def fused(features, labels, coeffs, smoothing, pair_slots):
    width, rows = features.shape
    slab = width // 8
    half = rows // 2
    places = jnp.array(slot_places() + [N_OFF + CLASSES], jnp.int32)
    i16 = jnp.int16
    sem = pltpu.SemaphoreType.DMA
    n = N_CHUNKS
    scratch = [
        pltpu.VMEM((width, rows), bf16),
        pltpu.VMEM((rows, width), bf16),
        pltpu.VMEM((2, width, half), bf16),
        pltpu.VMEM((2, half, width), bf16),
        pltpu.VMEM((2, 8, 2 * width), f32),
        pltpu.VMEM((CLASSES, 2 * width), f32),
        pltpu.VMEM((2, CLASSES, rows), f32),
        pltpu.VMEM((N_OFF, rows), f32),
        pltpu.VMEM((CLASSES, rows), bf16),
        pltpu.VMEM((n, GROUP, 2, 2, 2, slab, width), f32),
        pltpu.VMEM((n, GROUP, 2, 2, slab, width), f32),
        pltpu.VMEM((n, GROUP, 2, slab, width), f32),
        pltpu.VMEM((n, GROUP, 2, slab, width), i16),
        pltpu.VMEM((n, GROUP, width), f32),
        pltpu.VMEM((n, GROUP, 2, slab, width), i16),
        pltpu.VMEM((n, GROUP, width), f32),
        pltpu.VMEM((n, GROUP, slab, width), f32),
        pltpu.VMEM((n, GROUP, slab, width), i16),
        pltpu.VMEM((n, GROUP, width), f32),
        pltpu.VMEM((n, GROUP, slab, width), i16),
        pltpu.VMEM((n, GROUP, width), f32),
        pltpu.VMEM((n, GROUP, slab, width), f32),
        pltpu.VMEM((n, GROUP, slab, width), i16),
        pltpu.VMEM((n, GROUP, width), f32),
        pltpu.VMEM((n, GROUP, slab, width), i16),
        pltpu.VMEM((n, GROUP, width), f32),
        pltpu.VMEM((n, GROUP, slab, width), i16),
        pltpu.VMEM((n, GROUP, width), f32),
        pltpu.VMEM((n, GROUP, slab, width), i16),
        pltpu.VMEM((n, GROUP, width), f32),
        pltpu.VMEM((N_OFF + CLASSES + 1, slab, width), f32),
        pltpu.VMEM((N_OFF + CLASSES + 1, slab, width), f32),
        pltpu.VMEM((N_PACKS, width, LANES), i16),
        pltpu.VMEM((N_PACKS, 1, LANES), f32),
        pltpu.VMEM((N_PACKS, 8, slab, LANES), i16),
        pltpu.VMEM((N_PACKS, 8, 1, LANES), f32),
        pltpu.VMEM((5, CLASSES, width), f32),
        pltpu.VMEM((5, CLASSES, width), f32),
        sem, sem((2,)), sem((2,)), sem((2,)),
        sem((n + 1,)), sem((n + 1,)), sem((n + 1,)), sem((n + 1,)), sem((n + 1,)),
        sem((2, n)), sem((2, n)), sem((2, n)), sem((2, n)),
        sem((2, N_PACKS)), sem((2, N_PACKS)), sem((2, 5)),
    ]
    vmem = pl.BlockSpec(memory_space=pltpu.VMEM)
    smem = pl.BlockSpec(memory_space=pltpu.SMEM)
    return pl.pallas_call(
        kernel_body,
        out_shape=(
            jax.ShapeDtypeStruct((slab, pair_slots.shape[0], 2 * width), f32),
            jax.ShapeDtypeStruct((coeffs.shape[0], slab), f32),
        ),
        in_specs=[pl.BlockSpec(memory_space=pl.ANY), vmem, vmem, smem, smem, smem],
        out_specs=(vmem, vmem),
        scratch_shapes=scratch,
        compiler_params=pltpu.CompilerParams(
            collective_id=0, has_side_effects=True, vmem_limit_bytes=64 * 2**20 - 65536
        ),
        name="newton",
    )(features, labels.reshape(1, rows), coeffs, smoothing, pair_slots, places)


def step(features, labels, coeffs, smoothing, pair_slots):
    width = features.shape[0]
    fits = lax.axis_size("cls") == 2 and lax.axis_size("dp") == 16
    fits = fits and (width // 8) * PACK == LANES and N_OFF % PACK == 0
    fits = fits and features.shape[1] % 1024 == 0
    run = fused if fits else local
    return run(features, labels, coeffs, smoothing, pair_slots)


def solution(mesh):
    return jax.shard_map(
        step,
        mesh=mesh,
        in_specs=(P("cls", "dp"), P("dp"), P("cls", None), P(), P("cls")),
        out_specs=(P("dp", "cls", None), P("cls", "dp")),
        check_vma=False,
    )
```
